512 devices in a mesh: seed: 2 (over core), dp: 4 (over x), tensor: 64 (over z, y).
Axes of the slice: x: 4, y: 8, z: 8, core: 2. Of those that a mesh axis runs over, the one named last changes fastest.
Arguments:
- hidden: bfloat16 [2, 64, 96, 2048], P('seed', 'dp', None, 'tensor'), may hold values from -24 to 24
- norm_gain: float32 [2, 2048], P('seed'), may hold values from 0.25 to 1.75
- lm_head: bfloat16 [2, 2048, 65536], P('seed', None, 'tensor'), may hold values from -3 to 3
- targets: int32 [64, 96], P('dp'), may hold values from 0 to 65535
- lengths: int32 [64], P('dp'), may hold values from 24 to 96
Outputs:
- token_scores: float32 [2, 64, 96], P('seed', 'dp')
- ensemble: float32 [64], P('dp')
- centered: float32 [64], P('dp')
The draws below stay inside these ranges and needn't reach their ends.
All inputs are finite; a program needn't handle non-finite values.
Results may differ from the reference program's by a relative error of at most 0.0003.
The reference program's roundings to bfloat16 on the way (of `normed`) count: a program that leaves them out, or rounds other values in their place, can miss the bound.
Values may be sent and summed in bfloat16 or wider, within the bound.
A program may use at most 128 MiB of HBM per device.

```python
import math
import jax
import jax.numpy as jnp
from jax import lax

D = 2048
VOCAB = 65536
SEQ = 96
EXAMPLES = 64
SEEDS = 2


plain_scale = 3.0


def shared_chosen(key):
    return jax.random.randint(jax.random.fold_in(key, 19), (EXAMPLES * 2,), 0, VOCAB, dtype=jnp.int32)


def shared_head(key):
    base = jax.random.normal(jax.random.fold_in(key, 11), (SEEDS, D, VOCAB), jnp.float32)
    plain = jnp.clip(base, -6.0, 6.0) * (plain_scale / math.sqrt(D))
    chosen = shared_chosen(key)
    strong = jnp.clip(jnp.take(base, chosen, axis=2) * (260.0 / D), -3.0, 3.0)
    return plain.at[:, :, chosen].set(strong)


def shared_targets(key):
    return jax.random.randint(jax.random.fold_in(key, 13), (EXAMPLES, SEQ), 0, VOCAB, dtype=jnp.int32)


def draw_lm_head(key, part):
    return shared_head(key).astype(jnp.bfloat16)


def draw_targets(key, part):
    return shared_targets(key)


def draw_hidden(key, part):
    head = shared_head(key)
    wanted = shared_targets(key)
    chosen = shared_chosen(key)
    stretch = math.sqrt(D) / plain_scale
    along = jnp.take(head, wanted.reshape(-1), axis=2)
    along = jnp.transpose(along, (0, 2, 1)).reshape(SEEDS, EXAMPLES, SEQ, D) * stretch
    along = jnp.clip(along, -4.0, 4.0)
    level = jax.random.uniform(jax.random.fold_in(key, 17), (SEEDS, EXAMPLES, 1, 1), jnp.float32, 0.0, 0.12)
    wobble = jax.random.uniform(jax.random.fold_in(key, 29), (SEEDS, EXAMPLES, SEQ, 1), jnp.float32, 0.6, 1.0)
    strength = level * wobble
    aligned = jnp.take(head, chosen, axis=2)
    aligned = jnp.transpose(aligned, (0, 2, 1)).reshape(SEEDS, EXAMPLES, 2, D) * (math.sqrt(D) / 5.5)
    early = SEQ // 4
    first_spot = jax.random.randint(jax.random.fold_in(key, 31), (SEEDS, EXAMPLES, 1), 0, early, dtype=jnp.int32)
    offset_spot = jax.random.randint(jax.random.fold_in(key, 37), (SEEDS, EXAMPLES, 1), 0, early - 1, dtype=jnp.int32)
    second_spot = (first_spot + 1 + offset_spot) % early
    position = jnp.arange(SEQ, dtype=jnp.int32)[None, None, :]
    first_mask = (position == first_spot)[:, :, :, None]
    second_mask = (position == second_spot)[:, :, :, None]
    noise = jnp.clip(jax.random.normal(jax.random.fold_in(key, 21), (SEEDS, EXAMPLES, SEQ, D), jnp.float32), -5.0, 5.0)
    mixed = noise + strength * along
    mixed = jnp.where(first_mask, aligned[:, :, 0:1, :], mixed)
    mixed = jnp.where(second_mask, aligned[:, :, 1:2, :], mixed)
    return mixed.astype(jnp.bfloat16)


def with_ends(result, stream_key, smallest, high):
    extent = result.shape
    index_at = [jax.random.randint(jax.random.fold_in(stream_key, axis), (), 0, extent[axis]) for axis in range(len(extent))]
    result = result.at[tuple(index_at)].set(smallest)
    longest = extent.index(max(extent))
    index_at[longest] = (index_at[longest] + 1) % extent[longest]
    return result.at[tuple(index_at)].set(high)


def setup_inputs(seed: int = 0) -> dict:
    keys = jax.random.split(jax.random.key(seed), 6)
    hidden = draw_hidden(jax.random.fold_in(keys[5], 71), 0)
    norm_gain = jnp.clip(1.0 + 0.15 * jax.random.normal(keys[1], (SEEDS, D), jnp.float32), 0.25, 1.75)
    lm_head = draw_lm_head(jax.random.fold_in(keys[5], 71), 0)
    targets = draw_targets(jax.random.fold_in(keys[5], 71), 0)
    lengths = with_ends(jax.random.randint(keys[4], (EXAMPLES,), SEQ // 4, SEQ + 1), jax.random.fold_in(keys[4], 1), SEQ // 4, SEQ).astype(jnp.int32)
    return dict(hidden=hidden, norm_gain=norm_gain, lm_head=lm_head, targets=targets, lengths=lengths)


rms_epsilon = 1e-05

def score_example(rows, gain, weight, wanted):
    flat = rows.astype(jnp.float32)
    mean_sq = lax.optimization_barrier(jnp.mean(flat * flat, axis=1, keepdims=True))
    normed = (flat * lax.rsqrt(mean_sq + rms_epsilon) * gain).astype(jnp.bfloat16)
    logits = jnp.dot(normed, weight, preferred_element_type=jnp.float32)
    top_value = lax.optimization_barrier(jnp.max(logits, axis=1, keepdims=True))
    scaled_exp = jnp.exp(logits - top_value)
    probability = scaled_exp / lax.optimization_barrier(jnp.sum(scaled_exp, axis=1, keepdims=True))
    column = jnp.arange(logits.shape[1], dtype=jnp.int32)
    onehot = (column[None, :] == wanted[:, None]).astype(jnp.float32)
    distance = probability - onehot
    return jnp.sqrt(lax.optimization_barrier(jnp.sum(distance * distance, axis=1)))

def reference(hidden, norm_gain, lm_head, targets, lengths):

    def per_seed(member):
        states, gain, weight = member
        return lax.map(lambda pair: score_example(pair[0], gain, weight, pair[1]), (states, targets))
    scores = lax.map(per_seed, (hidden, norm_gain.astype(jnp.float32), lm_head))
    position = jnp.arange(SEQ, dtype=jnp.int32)
    valid = position[None, :] < lengths[:, None]
    token_scores = jnp.where(valid[None, :, :], scores, jnp.float32(0.0))
    example_scores = lax.optimization_barrier(jnp.sum(token_scores, axis=2)) / lengths.astype(jnp.float32)[None, :]
    ensemble = lax.optimization_barrier(jnp.sum(example_scores, axis=0)) / SEEDS
    centered = ensemble - jnp.sum(ensemble) / EXAMPLES
    return (token_scores, ensemble, centered)
```

```python
import functools

import jax
import jax.numpy as jnp
from jax import lax
from jax.experimental import pallas as pl
from jax.experimental.pallas import tpu as pltpu
from jax.sharding import Mesh
from jax.sharding import PartitionSpec as P

MESH = pl.DeviceIdType.MESH
TENSOR = ("tensor_0", "tensor_1")
LANES = 128
RMS_EPSILON = 1e-05


def kernel(
    sizes,
    hidden_hbm,
    gain_hbm,
    weight_hbm,
    target_hbm,
    length_ref,
    token_ref,
    ensemble_ref,
    centered_ref,
    gathered,
    hidden_own,
    gain_own,
    weight_own,
    target_own,
    weight_turned,
    gain_wide,
    target_lanes,
    logits,
    normed,
    stats_y,
    stats_z,
    scores,
    examples,
    load_sem,
    send_sem,
    recv_sem,
    stat_send,
    stat_recv,
    end_send,
    end_recv,
):
    ring, members, groups, batch, seq, width = sizes
    half_ring = ring // 2
    chunks = gathered.shape[0]
    units = chunks // 2
    depth = gathered.shape[1] * gathered.shape[2] * width
    vocab = weight_own.shape[1]
    s, d = lax.axis_index("seed"), lax.axis_index("dp")
    z, y = lax.axis_index("tensor_0"), lax.axis_index("tensor_1")

    def along_z(k):
        return lax.rem(z + (k + ring), ring)

    def along_y(k):
        return lax.rem(y + (k + ring), ring)

    barrier = pltpu.get_barrier_semaphore()
    others = [(a, b) for a in range(members) for b in range(groups) if a or b]
    for k in range(1, ring):
        pl.semaphore_signal(barrier, inc=1, device_id={"tensor_0": along_z(k)}, device_id_type=MESH)
        pl.semaphore_signal(barrier, inc=1, device_id={"tensor_1": along_y(k)}, device_id_type=MESH)
    for a, b in others:
        pl.semaphore_signal(
            barrier,
            inc=1,
            device_id={"seed": lax.rem(s + a, members), "dp": lax.rem(d + b, groups)},
            device_id_type=MESH,
        )
    loads = [
        pltpu.make_async_copy(hidden_hbm, hidden_own, load_sem.at[0]),
        pltpu.make_async_copy(target_hbm, target_own, load_sem.at[1]),
        pltpu.make_async_copy(gain_hbm, gain_own, load_sem.at[2]),
        pltpu.make_async_copy(weight_hbm, weight_own, load_sem.at[3]),
    ]
    for load in loads:
        load.start()

    loads[0].wait()
    for q in range(batch // 4):
        part = [hidden_own[4 * q + r].astype(jnp.float32) for r in range(4)]
        joined = lanes_joined(part)
        for r in range(3):
            gathered[3 * q + r, z, y] = joined[r].astype(jnp.bfloat16)
    pl.semaphore_wait(barrier, 2 * (ring - 1) + len(others))

    pending = []
    count = [0]

    def message(view, at, axis, sign):
        number = count[0]
        count[0] += 1
        step = (sign, 0) if axis == 0 else (0, sign)
        device = {"tensor_0": along_z(sign)} if axis == 0 else {"tensor_1": along_y(sign)}

        def copy(place):
            return pltpu.make_async_remote_copy(
                src_ref=view(*place),
                dst_ref=view(*place),
                send_sem=send_sem.at[number],
                recv_sem=recv_sem.at[number],
                device_id=device,
                device_id_type=MESH,
            )

        sent = copy(at)
        sent.start()
        pending.append(sent)
        return copy((at[0] - step[0], at[1] - step[1])), (at[0] - step[0], at[1] - step[1])

    def shard_view(kind, first, number):
        def view(dz, dy):
            return gathered.at[pl.ds(kind * units + first, number), along_z(dz), along_y(dy)]

        return view

    def block_view(kind, unit, part):
        def view(dz, dy):
            if kind == 0:
                return gathered.at[unit, along_z(dz), pl.ds(*part)]
            return gathered.at[units + unit, pl.ds(*part), along_y(dy)]

        return view

    first_axis = {0: 1, 1: 0}
    whole = (0, units)
    halves = {1: (0, units // 2), -1: (units // 2, units - units // 2)}
    phase_one = {}
    arriving = []
    for kind in (0, 1):
        for sign in (1, -1):
            phase_one[kind, sign] = message(shard_view(kind, *whole), (0, 0), first_axis[kind], sign)
    for kind in (0, 1):
        for sign in (1, -1):
            arriving.append(message(shard_view(kind, *whole), (0, 0), 1 - first_axis[kind], sign)[0])

    prepared = [0]

    def prepare(upto):
        while prepared[0] < min(upto, depth // 256):
            k = prepared[0]
            if k == 0:
                loads[1].wait()
                loads[2].wait()
                loads[3].wait()
                for q in range(batch // 4):
                    part = [target_own[pl.ds(4 * q + r, 1), :] for r in range(4)]
                    joined = lanes_joined(part)
                    for r in range(3):
                        target_lanes[pl.ds(3 * q + r, 1), :] = joined[r]
                for b in range(depth // LANES):
                    row = gain_own[:, b * LANES : (b + 1) * LANES]
                    gain_wide[b * LANES : (b + 1) * LANES, :] = jnp.broadcast_to(
                        row, (LANES, LANES)
                    ).T
            for v in range(vocab // 256):
                block = weight_own[k * 256 : (k + 1) * 256, v * 256 : (v + 1) * 256]
                weight_turned[v * 256 : (v + 1) * 256, k * 256 : (k + 1) * 256] = block.T
            prepared[0] += 1

    for step in range(1, half_ring + 1):
        prepare(step * depth // 256 // half_ring)
        places = {}
        for kind in (0, 1):
            for sign in (1, -1):
                copy, at = phase_one[kind, sign]
                copy.wait_recv()
                places[kind, sign] = at
                if step < half_ring:
                    span = whole if step + 1 < half_ring else halves[sign]
                    phase_one[kind, sign] = message(
                        shard_view(kind, *span), at, first_axis[kind], sign
                    )
        for kind in (0, 1):
            for sign in (1, -1) if step < half_ring else (1,):
                for way in (1, -1):
                    arriving.append(
                        message(
                            shard_view(kind, *whole), places[kind, sign], 1 - first_axis[kind], way
                        )[0]
                    )
    for copy in arriving:
        copy.wait_recv()

    def unit_stats(u):
        for side, c in enumerate((u, units + u)):
            total = jnp.zeros((1, LANES), jnp.float32)
            for b in range(depth // 256):
                x = gathered[c, b].reshape(256, LANES).astype(jnp.float32)
                total += jnp.sum(x * x, axis=0, keepdims=True)
            scale = lax.rsqrt(total * (1.0 / depth) + RMS_EPSILON)
            for b in range(depth // 256):
                x = gathered[c, b].reshape(256, LANES).astype(jnp.float32)
                gain = gain_wide[b * 256 : (b + 1) * 256, :]
                normed[b * 256 : (b + 1) * 256, side * LANES : (side + 1) * LANES] = (
                    x * scale * gain
                ).astype(jnp.bfloat16)
        for v in range(vocab // 256):
            logits[v * 256 : (v + 1) * 256, :] = jnp.dot(
                weight_turned[v * 256 : (v + 1) * 256, :],
                normed[...],
                preferred_element_type=jnp.float32,
            )
        own_first = (z * ring + y) * vocab
        rows = []
        for side, c in enumerate((u, units + u)):
            block = logits[:, side * LANES : (side + 1) * LANES]
            top = jnp.max(block, axis=0, keepdims=True)
            wanted = target_lanes[pl.ds(c, 1), :] - own_first
            column = lax.broadcasted_iota(jnp.int32, (vocab, LANES), 0)
            scaled = jnp.exp(block - top)
            hit = column == wanted
            other = jnp.where(hit, 0.0, scaled)
            rows.append(
                (
                    top,
                    jnp.sum(other, axis=0, keepdims=True),
                    jnp.sum(other * other, axis=0, keepdims=True),
                    jnp.sum(jnp.where(hit, scaled, 0.0), axis=0, keepdims=True),
                )
            )
        return jnp.concatenate([rows[side][k] for k in range(4) for side in range(2)], axis=0)

    def stat_copy(buffer, u, level, k):
        if level == 0:
            device, mine = {"tensor_1": along_y(k)}, y
        else:
            device, mine = {"tensor_0": along_z(k)}, z

        def copy(place):
            return pltpu.make_async_remote_copy(
                src_ref=buffer.at[u, place],
                dst_ref=buffer.at[u, place],
                send_sem=stat_send.at[u, level, k],
                recv_sem=stat_recv.at[u, level, k],
                device_id=device,
                device_id_type=MESH,
            )

        back = lax.rem(mine + (ring - k), ring)
        return copy(mine), copy(back)

    arrivals = {}

    def share(buffer, u, level, value):
        buffer[u, y if level == 0 else z] = value
        arrivals[u, level] = []
        for k in sorted(range(1, ring), key=lambda k: -min(k, ring - k)):
            sent, back = stat_copy(buffer, u, level, k)
            sent.start()
            pending.append(sent)
            arrivals[u, level].append(back)

    def combined(buffer, u, level):
        for copy in arrivals[u, level]:
            copy.wait_recv()
        parts = buffer[u]
        tops = parts[:, 0:2]
        top = jnp.max(tops, axis=0)
        scale = jnp.exp(tops - top[None])
        return jnp.concatenate(
            [
                top,
                jnp.sum(parts[:, 2:4] * scale, axis=0),
                jnp.sum(parts[:, 4:6] * scale * scale, axis=0),
                jnp.sum(parts[:, 6:8] * scale, axis=0),
            ],
            axis=0,
        )

    def finish(u):
        value = combined(stats_z, u, 1)
        other, square, wanted = (value[2:4], value[4:6], value[6:8])
        score = jnp.sqrt(other * other + square) / (other + wanted)
        scores[pl.ds(u, 1), :] = score[0:1]
        scores[pl.ds(units + u, 1), :] = score[1:2]

    hops = {}
    last = half_ring - 1
    for slot in range(units + last + 2):
        for hop in range(2, half_ring + 1):
            unit = slot - (hop - 2)
            if not 0 <= unit < units:
                continue
            for kind in (0, 1):
                for sign in (1, -1):
                    if hop == 2:
                        at = (-sign, 0) if kind == 0 else (0, -sign)
                    else:
                        copy, at = hops[kind, sign, unit]
                        copy.wait_recv()
                    part = (0, ring)
                    if hop == half_ring:
                        part = (0, half_ring) if sign == 1 else (half_ring, ring - half_ring)
                    hops[kind, sign, unit] = message(
                        block_view(kind, unit, part), at, 1 - first_axis[kind], sign
                    )
        unit = slot - last
        if 0 <= unit < units:
            for kind in (0, 1):
                for sign in (1, -1):
                    hops[kind, sign, unit][0].wait_recv()
            share(stats_y, unit, 0, unit_stats(unit))
        if 0 <= unit - 1 < units:
            share(stats_z, unit - 1, 1, combined(stats_y, unit - 1, 0))
        if 0 <= unit - 2 < units:
            finish(unit - 2)

    for q in range(batch // 4):
        part = [scores[pl.ds(3 * q + r, 1), :] for r in range(3)]
        split = [
            part[0][:, :seq],
            jnp.concatenate([part[0][:, 96:], part[1][:, :64]], axis=1),
            jnp.concatenate([part[1][:, 64:], part[2][:, :32]], axis=1),
            part[2][:, 32:],
        ]
        for r in range(4):
            token_ref[pl.ds(4 * q + r, 1), :] = split[r]
    example = lax.broadcasted_iota(jnp.int32, (batch, seq), 0)
    length = jnp.zeros((batch, seq), jnp.int32)
    for b in range(batch):
        length = jnp.where(example == b, length_ref[b], length)
    position = lax.broadcasted_iota(jnp.int32, (batch, seq), 1)
    token = jnp.where(position < length, token_ref[...], 0.0)
    token_ref[...] = token
    mean = jnp.sum(token, axis=1, keepdims=True) / length.astype(jnp.float32)[:, :1]
    examples[s * groups + d] = jnp.broadcast_to(mean, (batch, LANES))

    waiting = []
    for a, b in others:

        def copy(place):
            return pltpu.make_async_remote_copy(
                src_ref=examples.at[place],
                dst_ref=examples.at[place],
                send_sem=end_send.at[a, b],
                recv_sem=end_recv.at[a, b],
                device_id={"seed": lax.rem(s + a, members), "dp": lax.rem(d + b, groups)},
                device_id_type=MESH,
            )

        sent = copy(s * groups + d)
        sent.start()
        pending.append(sent)
        waiting.append(
            copy(lax.rem(s + members - a, members) * groups + lax.rem(d + groups - b, groups))
        )
    for copy in waiting:
        copy.wait_recv()
    total = jnp.zeros((batch, LANES), jnp.float32)
    own = jnp.zeros((batch, LANES), jnp.float32)
    for b in range(groups):
        pair = examples[b]
        for a in range(1, members):
            pair += examples[a * groups + b]
        pair = pair * (1.0 / members)
        total += pair
        own = jnp.where(d == b, pair, own)
    average = jnp.sum(total, axis=0, keepdims=True) * (1.0 / (groups * batch))
    row = lax.broadcasted_iota(jnp.int32, (batch, LANES), 0)
    lane = lax.broadcasted_iota(jnp.int32, (batch, LANES), 1)
    ensemble = jnp.sum(jnp.where(row == lane, own, 0.0), axis=0, keepdims=True)
    ensemble_ref[...] = ensemble[:, :batch]
    centered_ref[...] = (ensemble - average)[:, :batch]
    for copy in pending:
        copy.wait_send()


def lanes_joined(part):
    return (
        jnp.concatenate([part[0], part[1][:, :32]], axis=1),
        jnp.concatenate([part[1][:, 32:], part[2][:, :64]], axis=1),
        jnp.concatenate([part[2][:, 64:], part[3]], axis=1),
    )


def shards(ring, members, groups, hidden, norm_gain, lm_head, targets, lengths):
    batch, seq, width = hidden.shape[1:]
    depth, vocab = lm_head.shape[1:]
    chunks = batch * seq // LANES
    units = chunks // 2
    half = ring // 2
    messages = 4 * half + 4 * (2 * half) + 4 * (half - 1) * units
    far = pl.BlockSpec(memory_space=pltpu.HBM)
    vmem = pl.BlockSpec(memory_space=pltpu.VMEM)
    f32 = jnp.float32
    token, ensemble, centered = pl.pallas_call(
        functools.partial(kernel, (ring, members, groups, batch, seq, width)),
        out_shape=(
            jax.ShapeDtypeStruct((batch, seq), f32),
            jax.ShapeDtypeStruct((1, batch), f32),
            jax.ShapeDtypeStruct((1, batch), f32),
        ),
        in_specs=[far] * 4 + [pl.BlockSpec(memory_space=pltpu.SMEM)],
        out_specs=(vmem, vmem, vmem),
        scratch_shapes=[
            pltpu.VMEM((chunks, ring, ring, width, LANES), jnp.bfloat16),
            pltpu.VMEM((batch, width, seq), jnp.bfloat16),
            pltpu.VMEM((1, depth), f32),
            pltpu.VMEM((depth, vocab), jnp.bfloat16),
            pltpu.VMEM((batch, seq), jnp.int32),
            pltpu.VMEM((vocab, depth), jnp.bfloat16),
            pltpu.VMEM((depth, LANES), f32),
            pltpu.VMEM((chunks, LANES), jnp.int32),
            pltpu.VMEM((vocab, 2 * LANES), f32),
            pltpu.VMEM((depth, 2 * LANES), jnp.bfloat16),
            pltpu.VMEM((units, ring, 8, LANES), f32),
            pltpu.VMEM((units, ring, 8, LANES), f32),
            pltpu.VMEM((chunks, LANES), f32),
            pltpu.VMEM((members * groups, batch, LANES), f32),
            pltpu.SemaphoreType.DMA((4,)),
            pltpu.SemaphoreType.DMA((messages,)),
            pltpu.SemaphoreType.DMA((messages,)),
            pltpu.SemaphoreType.DMA((units, 2, ring)),
            pltpu.SemaphoreType.DMA((units, 2, ring)),
            pltpu.SemaphoreType.DMA((members, groups)),
            pltpu.SemaphoreType.DMA((members, groups)),
        ],
        compiler_params=pltpu.CompilerParams(
            collective_id=0, has_side_effects=True, vmem_limit_bytes=67043328
        ),
    )(
        hidden[0].transpose(0, 2, 1),
        norm_gain,
        lm_head[0],
        targets,
        lengths,
    )
    return token[None], ensemble[0], centered[0]


def solution(mesh):
    ring = 8
    finer = Mesh(
        mesh.devices.reshape(mesh.shape["seed"], mesh.shape["dp"], ring, ring),
        ("seed", "dp", "tensor_0", "tensor_1"),
    )
    in_specs = (
        P("seed", "dp", None, TENSOR),
        P("seed", None),
        P("seed", None, TENSOR),
        P("dp", None),
        P("dp"),
    )
    out_specs = (P("seed", "dp", None), P("dp"), P("dp"))
    return jax.shard_map(
        functools.partial(shards, ring, mesh.shape["seed"], mesh.shape["dp"]),
        mesh=finer,
        in_specs=in_specs,
        out_specs=out_specs,
        check_vma=False,
    )
```

```python
import functools

import jax
import jax.numpy as jnp
from jax import lax
from jax.experimental import pallas as pl
from jax.experimental.pallas import tpu as pltpu
from jax.sharding import Mesh
from jax.sharding import PartitionSpec as P

MESH = pl.DeviceIdType.MESH
TENSOR = ("tensor_0", "tensor_1")
LANES = 128
RMS_EPSILON = 1e-05
RING = 8
FIRST, SECOND, THIRD, FOURTH, FIFTH, PREPARE, UNIT = range(7)
OWNED = 3

GROUPS = ((0, 1), (1, 2), (3, 3))
ORDER = (
    (0, 0, 1), (0, 1, 1), (5, 0, 0), (0, 2, 1), (5, 1, 0), (1, 0, 0), (1, 1, 0), (5, 2, 0),
    (1, 2, 0), (5, 3, 0), (0, 0, 2), (1, 0, -1), (1, 0, 1), (0, 1, 2), (1, 1, -1), (1, 1, 1),
    (0, 2, 2), (2, 0, 0), (1, 2, -1), (1, 2, 1), (0, 0, 3), (1, 0, -2), (1, 0, 2), (2, 0, -1),
    (0, 1, 3), (1, 1, -2), (1, 1, 2), (2, 0, 1), (0, 2, 3), (1, 2, -2), (1, 2, 2), (0, 0, 4),
    (1, 0, -3), (1, 0, 3), (2, 0, -2), (0, 1, 4), (1, 1, -3), (1, 1, 3), (2, 0, 2), (2, 1, -1),
    (0, 2, 4), (1, 2, -3), (1, 2, 3), (1, 0, 4), (2, 0, -3), (2, 0, 3), (1, 1, 4), (2, 1, -2),
    (2, 1, -3), (2, 1, 0), (2, 1, 1), (1, 2, 4), (2, 1, 2), (2, 1, 3), (2, 0, 4), (2, 2, -1),
    (2, 1, 4), (2, 2, -2), (2, 2, -3), (2, 2, 0), (2, 2, 1), (2, 2, 2), (3, 0, 0), (2, 2, 3),
    (2, 2, 4), (3, 1, 0), (3, 2, 0), (4, 0, 0), (3, 3, 0), (4, 1, 0), (3, 4, 0), (6, 0, 0),
    (4, 2, 0), (6, 0, 1), (3, 5, 0), (6, 0, 2), (6, 1, 0), (4, 3, 0), (6, 1, 1), (4, 4, 0),
    (6, 1, 2), (6, 2, 0), (6, 2, 1), (4, 5, 0), (6, 2, 2), (6, 3, 0), (6, 3, 1), (6, 3, 2),
    (6, 4, 0), (6, 4, 1), (6, 4, 2), (6, 5, 0), (6, 5, 1), (6, 5, 2),
)

def kernel(
    sizes,
    hidden_hbm,
    gain_hbm,
    weight_hbm,
    target_hbm,
    length_hbm,
    token_hbm,
    ensemble_hbm,
    centered_hbm,
    gathered,
    hidden_own,
    gain_own,
    weight_own,
    target_own,
    length_own,
    weight_turned,
    gain_wide,
    target_lanes,
    logits,
    normed,
    part,
    owned_y,
    owned_z,
    owned_score,
    stats_y,
    stats_z,
    scores,
    examples,
    token_out,
    ensemble_out,
    centered_out,
    load_sem,
    send_sem,
    recv_sem,
    stat_sem,
    end_sem,
):
    ring, members, groups, batch, seq, width = sizes
    chunks = gathered.shape[0]
    units = chunks // 2
    depth = ring * ring * width
    vocab = weight_own.shape[1]
    s, d = lax.axis_index("seed"), lax.axis_index("dp")
    z, y = lax.axis_index("tensor_0"), lax.axis_index("tensor_1")

    def along_z(k):
        return lax.rem(z + (k + ring), ring)

    def along_y(k):
        return lax.rem(y + (k + ring), ring)

    loads = [
        pltpu.make_async_copy(hidden_hbm, hidden_own, load_sem.at[0]),
        pltpu.make_async_copy(target_hbm, target_own, load_sem.at[1]),
        pltpu.make_async_copy(gain_hbm, gain_own, load_sem.at[2]),
        pltpu.make_async_copy(length_hbm, length_own, load_sem.at[3]),
        pltpu.make_async_copy(weight_hbm, weight_own, load_sem.at[4]),
    ]
    loads[0].start()
    barrier = pltpu.get_barrier_semaphore()
    others = [(a, b) for a in range(members) for b in range(groups) if a or b]
    for k in (1, -1):
        pl.semaphore_signal(barrier, inc=1, device_id={"tensor_0": along_z(k)}, device_id_type=MESH)
        pl.semaphore_signal(barrier, inc=1, device_id={"tensor_1": along_y(k)}, device_id_type=MESH)
    for a, b in others:
        pl.semaphore_signal(
            barrier,
            inc=1,
            device_id={"seed": lax.rem(s + a, members), "dp": lax.rem(d + b, groups)},
            device_id_type=MESH,
        )
    for load in loads[1:]:
        load.start()

    loads[0].wait()
    for q in range(batch // 4):
        joined = lanes_joined([hidden_own[4 * q + r].astype(jnp.float32) for r in range(4)])
        for r in range(3):
            gathered[3 * q + r, z, y] = joined[r].astype(jnp.bfloat16)
    pl.semaphore_wait(barrier, 4 + len(others))

    sides = [(kind, sign) for kind in (0, 1) for sign in (1, -1)]

    arrival = {}

    def send(key, view, at, axis, sign):
        what, g, k = key
        if key not in arrival:
            arrival[key] = len(arrival)
        pltpu.make_async_remote_copy(
            src_ref=view(*at),
            dst_ref=view(*at),
            send_sem=send_sem.at[5 if (what, k) == (FIRST, 4) else what],
            recv_sem=recv_sem.at[arrival[key]],
            device_id={"tensor_0": along_z(sign)} if axis == 0 else {"tensor_1": along_y(sign)},
            device_id_type=MESH,
        ).start()

    def bulk(ref, which, number):
        return pltpu.make_async_remote_copy(
            src_ref=ref,
            dst_ref=ref,
            send_sem=send_sem.at[which],
            recv_sem=recv_sem.at[number],
            device_id={"tensor_0": along_z(1)},
            device_id_type=MESH,
        )

    waited = set()

    def need(what, g, k):
        if (what, g, k) in waited:
            return
        waited.add((what, g, k))
        if what in (FIRST, SECOND):
            ref = gathered.at[pl.ds(0, GROUPS[g][1]), 0, pl.ds(0, 2 if (what, k) == (FIRST, 4) else 4)]
        elif what == THIRD:
            ref = gathered.at[pl.ds(0, GROUPS[g][1]), pl.ds(0, 4)]
        else:
            ref = gathered.at[0, pl.ds(0, 4 if what == FOURTH else 2)]
        bulk(ref, what, arrival[what, g, k]).wait_recv()

    def wait_sends():
        refs = (
            gathered.at[:, 0, pl.ds(0, 6)],
            gathered.at[:, pl.ds(0, 2)],
            gathered.at[:, pl.ds(0, 2)],
            gathered.at[:, pl.ds(0, 2)],
            gathered.at[:, 0],
            gathered.at[:, 0, pl.ds(0, 1)],
        )
        for which, ref in enumerate(refs):
            bulk(ref, which, 0).wait_send()

    def place(kind, first, second):
        return (second, first) if kind == 0 else (first, second)

    def shards_at(kind, g, piece):
        begin, number = GROUPS[g]

        def view(dz, dy):
            return gathered.at[
                pl.ds(kind * units + begin, number), along_z(dz), along_y(dy), pl.ds(*piece)
            ]

        return view

    def block_at(kind, c, piece):
        def view(dz, dy):
            if kind == 0:
                return gathered.at[c, along_z(dz), pl.ds(*piece)]
            return gathered.at[units + c, pl.ds(*piece), along_y(dy)]

        return view

    group_of = {
        c: g for g, (begin, number) in enumerate(GROUPS) for c in range(begin, begin + number)
    }

    def transfer(what, g, k):
        if what == FIRST:
            if k > 1:
                need(FIRST, g, k - 1)
        elif what == SECOND:
            if k:
                need(FIRST, g, abs(k))
        elif what == THIRD:
            need(SECOND, g, k)
        elif what == FOURTH:
            need(THIRD, group_of[g], 0)
        else:
            need(FOURTH, g, 0)
        for kind, sign in sides:
            first_axis = 1 if kind == 0 else 0
            if what == FIRST:
                piece = (0, width) if k < 4 else ((0, width // 2), (width // 2, width // 2))[sign < 0]
                at, axis = place(kind, -(k - 1) * sign, 0), first_axis
                view = shards_at(kind, g, piece)
            elif what in (SECOND, THIRD):
                at, axis = place(kind, k, 0 if what == SECOND else -sign), 1 - first_axis
                view = shards_at(kind, g, (0, width))
            elif what == FOURTH:
                at, axis = place(kind, 0, -2 * sign), 1 - first_axis
                view = block_at(kind, g, (0, ring))
            else:
                at, axis = place(kind, 0, -3 * sign), 1 - first_axis
                view = block_at(kind, g, ((0, ring // 2), (ring // 2, ring // 2))[sign < 0])
            send((what, g, 0 if what == THIRD else k), view, at, axis, sign)

    steps = 4

    def prepare(k):
        if k == 0:
            for load in loads[1:]:
                load.wait()
            for q in range(batch // 4):
                joined = lanes_joined([target_own[pl.ds(4 * q + r, 1), :] for r in range(4)])
                for r in range(3):
                    target_lanes[pl.ds(3 * q + r, 1), :] = joined[r]
            for b in range(depth // LANES):
                row = gain_own[:, b * LANES : (b + 1) * LANES]
                gain_wide[b * LANES : (b + 1) * LANES, :] = jnp.broadcast_to(row, (LANES, LANES)).T
            for j in range(2 * OWNED, ring):
                part[j] = jnp.ones(part.shape[1:], jnp.float32)
        for b in range(k * depth // 256 // steps, (k + 1) * depth // 256 // steps):
            for v in range(vocab // 256):
                block = weight_own[b * 256 : (b + 1) * 256, v * 256 : (v + 1) * 256]
                weight_turned[v * 256 : (v + 1) * 256, b * 256 : (b + 1) * 256] = block.T

    def normalize(u):
        for side, c in enumerate((u, units + u)):
            total = jnp.zeros((1, LANES), jnp.float32)
            for b in range(depth // 256):
                x = gathered[c, b].reshape(256, LANES).astype(jnp.float32)
                total += jnp.sum(x * x, axis=0, keepdims=True)
            scale = lax.rsqrt(total * (1.0 / depth) + RMS_EPSILON)
            for b in range(depth // 256):
                x = gathered[c, b].reshape(256, LANES).astype(jnp.float32)
                gain = gain_wide[b * 256 : (b + 1) * 256, :]
                normed[b * 256 : (b + 1) * 256, side * LANES : (side + 1) * LANES] = (
                    x * scale * gain
                ).astype(jnp.bfloat16)

    def multiply(u):
        own_first = (z * ring + y) * vocab
        row = lax.broadcasted_iota(jnp.int32, (256, 2 * LANES), 0)
        wanted = jnp.concatenate(
            [target_lanes[pl.ds(c, 1), :] for c in (u, units + u)], axis=1
        )
        tiles = vocab // 256
        found = []

        def dot(v):
            logits[v * 256 : (v + 1) * 256, :] = jnp.dot(
                weight_turned[v * 256 : (v + 1) * 256, :],
                normed[...],
                preferred_element_type=jnp.float32,
            )

        def stats(v):
            block = logits[v * 256 : (v + 1) * 256, :]
            top = jnp.max(block, axis=0, keepdims=True)
            scaled = jnp.exp(block - top)
            hit = row == wanted - (own_first + v * 256)
            other = jnp.where(hit, 0.0, scaled)
            found.append(
                (
                    top,
                    jnp.sum(other, axis=0, keepdims=True),
                    jnp.sum(other * other, axis=0, keepdims=True),
                    jnp.sum(jnp.where(hit, scaled, 0.0), axis=0, keepdims=True),
                )
            )

        dot(0)
        for v in range(1, tiles):
            dot(v)
            stats(v - 1)
        stats(tiles - 1)
        top = functools.reduce(jnp.maximum, [f[0] for f in found])
        scale = [jnp.exp(f[0] - top) for f in found]
        value = (
            top,
            sum(f[1] * e for f, e in zip(found, scale)),
            sum(f[2] * e * e for f, e in zip(found, scale)),
            sum(f[3] * e for f, e in zip(found, scale)),
        )
        return [[x[:, side * LANES : (side + 1) * LANES] for x in value] for side in range(2)]

    def merged(parts, wide):
        tops = parts[:, :wide]
        top = jnp.max(tops, axis=0)
        scale = jnp.exp(tops - top[None])
        return (
            top,
            jnp.sum(parts[:, wide : 2 * wide] * scale, axis=0),
            jnp.sum(parts[:, 2 * wide : 3 * wide] * scale * scale, axis=0),
            jnp.sum(parts[:, 3 * wide : 4 * wide] * scale, axis=0),
        )

    def score_of(value):
        top, other, square, wanted = value
        return jnp.sqrt(other * other + square) / (other + wanted)

    near = sorted(range(1, ring), key=lambda k: -min(k, ring - k))

    def exchange(level, slot, source, target):
        mine = y if level == 0 else z

        def copy(src, dst, k):
            return pltpu.make_async_remote_copy(
                src_ref=src,
                dst_ref=dst,
                send_sem=stat_sem.at[0, slot],
                recv_sem=stat_sem.at[1, slot],
                device_id={"tensor_1": along_y(k)} if level == 0 else {"tensor_0": along_z(k)},
                device_id_type=MESH,
            )

        for k in near:
            copy(source(k), target(mine), k).start()
        seven = part.at[pl.ds(0, ring - 1)]
        return copy(seven, seven, 1)

    def share(u, level, value):
        buffer = stats_y if level == 0 else stats_z
        i = u - OWNED
        buffer[i, y if level == 0 else z] = jnp.concatenate(value, axis=0)
        mine = y if level == 0 else z
        return exchange(
            level, 2 * i + level, lambda k: buffer.at[i, mine], lambda p: buffer.at[i, p]
        )

    def tile(value):
        rows = jnp.concatenate(value, axis=0)
        return jnp.concatenate([rows, jnp.zeros((8 - rows.shape[0], LANES), jnp.float32)], axis=0)

    base = 2 * (units - OWNED)
    back = {}

    def after(u, rows):
        if u < OWNED:
            part[u] = tile(rows[0])
            part[OWNED + u] = tile(rows[1])
            if u == OWNED - 1:
                owned_y[y] = part[y]
                back["owned", 0] = exchange(
                    0, base, lambda k: part.at[along_y(k)], lambda p: owned_y.at[p]
                )
            return
        value = [jnp.concatenate([rows[0][k], rows[1][k]], axis=0) for k in range(4)]
        back[u, 0] = share(u, 0, value)
        if u == units - 2:
            back["owned", 0].wait_recv()
            owned_z[z] = tile(merged(owned_y[...], 1))
            back["owned", 1] = exchange(
                1, base + 1, lambda k: owned_z.at[z], lambda p: owned_z.at[p]
            )

    def second_level(u):
        back[u, 0].wait_recv()
        back[u, 1] = share(u, 1, merged(stats_y[u - OWNED], 2))

    def finish(u):
        back[u, 1].wait_recv()
        score = score_of(merged(stats_z[u - OWNED], 2))
        scores[pl.ds(u, 1), :] = score[0:1]
        scores[pl.ds(units + u, 1), :] = score[1:2]

    for what, g, k in ORDER:
        if what == PREPARE:
            prepare(g)
        elif what == UNIT:
            if k == 0:
                need(FIFTH, g, 0)
                normalize(g)
            elif k == 1:
                after(g, multiply(g))
        else:
            transfer(what, g, k)
    for u in range(OWNED, units - 1):
        second_level(u)
    back["owned", 1].wait_recv()
    owned_score[y] = jnp.broadcast_to(score_of(merged(owned_z[...], 1)), (8, LANES))
    back["owned", 2] = exchange(
        0, base + 2, lambda k: owned_score.at[y], lambda p: owned_score.at[p]
    )
    second_level(units - 1)
    example = lax.broadcasted_iota(jnp.int32, (batch, seq), 0)
    length = jnp.zeros((batch, seq), jnp.int32)
    for b in range(batch):
        length = jnp.where(example == b, length_own[b], length)
    valid = lax.broadcasted_iota(jnp.int32, (batch, seq), 1) < length
    wait_sends()
    for u in range(OWNED, units - 1):
        finish(u)
    back["owned", 2].wait_recv()
    for u in range(OWNED):
        scores[pl.ds(u, 1), :] = owned_score[u, 0:1, :]
        scores[pl.ds(units + u, 1), :] = owned_score[OWNED + u, 0:1, :]
    finish(units - 1)

    for q in range(batch // 4):
        row = [scores[pl.ds(3 * q + r, 1), :] for r in range(3)]
        split = [
            row[0][:, :seq],
            jnp.concatenate([row[0][:, 96:], row[1][:, :64]], axis=1),
            jnp.concatenate([row[1][:, 64:], row[2][:, :32]], axis=1),
            row[2][:, 32:],
        ]
        for r in range(4):
            token_out[pl.ds(4 * q + r, 1), :] = split[r]
    token = jnp.where(valid, token_out[...], 0.0)
    token_out[...] = token
    mean = jnp.sum(token, axis=1, keepdims=True) / length.astype(jnp.float32)[:, :1]
    examples[s * groups + d] = jnp.broadcast_to(mean, (batch, LANES))

    def end_copy(src, dst, a, b):
        return pltpu.make_async_remote_copy(
            src_ref=src,
            dst_ref=dst,
            send_sem=end_sem.at[0],
            recv_sem=end_sem.at[1],
            device_id={"seed": lax.rem(s + a, members), "dp": lax.rem(d + b, groups)},
            device_id_type=MESH,
        )

    own_place = s * groups + d
    for a, b in others:
        end_copy(examples.at[own_place], examples.at[own_place], a, b).start()
    rest = examples.at[pl.ds(0, len(others))]
    stores = [pltpu.make_async_copy(token_out, token_hbm, load_sem.at[5])]
    stores[0].start()
    end_copy(rest, rest, *others[0]).wait_recv()
    total = jnp.zeros((batch, LANES), jnp.float32)
    own = jnp.zeros((batch, LANES), jnp.float32)
    for b in range(groups):
        pair = examples[b]
        for a in range(1, members):
            pair += examples[a * groups + b]
        pair = pair * (1.0 / members)
        total += pair
        own = jnp.where(d == b, pair, own)
    average = jnp.sum(total, axis=0, keepdims=True) * (1.0 / (groups * batch))
    row = lax.broadcasted_iota(jnp.int32, (batch, LANES), 0)
    lane = lax.broadcasted_iota(jnp.int32, (batch, LANES), 1)
    ensemble = jnp.sum(jnp.where(row == lane, own, 0.0), axis=0, keepdims=True)
    ensemble_out[...] = ensemble[:, :batch]
    centered_out[...] = (ensemble - average)[:, :batch]
    stores.append(pltpu.make_async_copy(ensemble_out, ensemble_hbm, load_sem.at[6]))
    stores.append(pltpu.make_async_copy(centered_out, centered_hbm, load_sem.at[7]))
    for store in stores[1:]:
        store.start()
    end_copy(rest, rest, *others[0]).wait_send()
    for copy in back.values():
        copy.wait_send()
    for store in stores:
        store.wait()


def lanes_joined(part):
    return (
        jnp.concatenate([part[0], part[1][:, :32]], axis=1),
        jnp.concatenate([part[1][:, 32:], part[2][:, :64]], axis=1),
        jnp.concatenate([part[2][:, 64:], part[3]], axis=1),
    )


def hand_over(*refs):
    count = len(refs) // 2
    copies = [
        pltpu.make_async_copy(refs[k], refs[count + k], refs[-1].at[k]) for k in range(count)
    ]
    for copy in copies:
        copy.start()
    for copy in copies:
        copy.wait()


def shards(members, groups, hidden, norm_gain, lm_head, targets, lengths):
    batch, seq, width = hidden.shape[1:]
    depth, vocab = lm_head.shape[1:]
    chunks = batch * seq // LANES
    units = chunks // 2
    direct = units - OWNED
    far = pl.BlockSpec(memory_space=pl.ANY)
    f32 = jnp.float32
    outs = (
        jax.ShapeDtypeStruct((batch, seq), f32),
        jax.ShapeDtypeStruct((1, batch), f32),
        jax.ShapeDtypeStruct((1, batch), f32),
    )
    result = pl.pallas_call(
        functools.partial(kernel, (RING, members, groups, batch, seq, width)),
        out_shape=outs,
        in_specs=[far] * 5,
        out_specs=(far, far, far),
        scratch_shapes=[
            pltpu.VMEM((chunks, RING, RING, width, LANES), jnp.bfloat16),
            pltpu.VMEM((batch, width, seq), jnp.bfloat16),
            pltpu.VMEM((1, depth), f32),
            pltpu.VMEM((depth, vocab), jnp.bfloat16),
            pltpu.VMEM((batch, seq), jnp.int32),
            pltpu.SMEM((batch,), jnp.int32),
            pltpu.VMEM((vocab, depth), jnp.bfloat16),
            pltpu.VMEM((depth, LANES), f32),
            pltpu.VMEM((chunks, LANES), jnp.int32),
            pltpu.VMEM((vocab, 2 * LANES), f32),
            pltpu.VMEM((depth, 2 * LANES), jnp.bfloat16),
            pltpu.VMEM((RING, 8, LANES), f32),
            pltpu.VMEM((RING, 8, LANES), f32),
            pltpu.VMEM((RING, 8, LANES), f32),
            pltpu.VMEM((RING, 8, LANES), f32),
            pltpu.VMEM((direct, RING, 8, LANES), f32),
            pltpu.VMEM((direct, RING, 8, LANES), f32),
            pltpu.VMEM((chunks, LANES), f32),
            pltpu.VMEM((members * groups, batch, LANES), f32),
            pltpu.VMEM((batch, seq), f32),
            pltpu.VMEM((1, batch), f32),
            pltpu.VMEM((1, batch), f32),
            pltpu.SemaphoreType.DMA((8,)),
            pltpu.SemaphoreType.DMA((6,)),
            pltpu.SemaphoreType.DMA((13 * len(GROUPS) + 2 * units,)),
            pltpu.SemaphoreType.DMA((2, 2 * direct + 3)),
            pltpu.SemaphoreType.DMA((2,)),
        ],
        compiler_params=pltpu.CompilerParams(
            collective_id=0, has_side_effects=True, vmem_limit_bytes=67043328
        ),
    )(
        hidden[0].transpose(0, 2, 1),
        norm_gain,
        lm_head[0],
        targets,
        lengths,
    )
    token, ensemble, centered = pl.pallas_call(
        hand_over,
        out_shape=outs,
        in_specs=[far] * 3,
        out_specs=(far, far, far),
        scratch_shapes=[pltpu.SemaphoreType.DMA((3,))],
    )(*result)
    return token[None], ensemble[0], centered[0]


def solution(mesh):
    finer = Mesh(
        mesh.devices.reshape(mesh.shape["seed"], mesh.shape["dp"], RING, RING),
        ("seed", "dp", "tensor_0", "tensor_1"),
    )
    in_specs = (
        P("seed", "dp", None, TENSOR),
        P("seed", None),
        P("seed", None, TENSOR),
        P("dp", None),
        P("dp"),
    )
    out_specs = (P("seed", "dp", None), P("dp"), P("dp"))
    return jax.shard_map(
        functools.partial(shards, mesh.shape["seed"], mesh.shape["dp"]),
        mesh=finer,
        in_specs=in_specs,
        out_specs=out_specs,
        check_vma=False,
    )
```

```python
import functools

import jax
import jax.numpy as jnp
from jax import lax
from jax.experimental import pallas as pl
from jax.experimental.pallas import tpu as pltpu
from jax.sharding import Mesh
from jax.sharding import PartitionSpec as P

MESH = pl.DeviceIdType.MESH
TENSOR = ("tensor_0", "tensor_1")
LANES = 128
RMS_EPSILON = 1e-05
RING = 8
FIRST, SECOND, THIRD, FOURTH, FIFTH, PREPARE, UNIT = range(7)
OWNED = 2

GROUPS = ((0, 2), (2, 4))
ORDER = (
    (0, 0, 1), (0, 1, 1), (5, 0, 0), (1, 1, 0), (5, 1, 0), (5, 2, 0), (1, 0, 0), (5, 3, 0),
    (0, 0, 2), (1, 0, -1), (1, 0, 1), (0, 1, 2), (1, 1, -1), (2, 0, 0), (2, 1, 0), (0, 0, 3),
    (2, 0, -1), (2, 0, 1), (1, 0, -2), (0, 1, 3), (1, 1, 2), (1, 1, -2), (0, 0, 4), (1, 0, 3),
    (1, 0, -3), (1, 0, 2), (2, 0, -2), (2, 1, -1), (0, 1, 4), (1, 1, 3), (1, 0, 4), (2, 0, 3),
    (2, 0, -3), (2, 0, 2), (1, 1, -3), (2, 1, 2), (1, 1, 4), (2, 0, 4), (2, 1, 3), (1, 1, 1),
    (2, 1, -3), (2, 1, -2), (2, 1, 4), (3, 0, 0), (2, 1, 1), (3, 1, 0), (4, 0, 0), (3, 2, 0),
    (3, 3, 0), (4, 1, 0), (6, 0, 0), (3, 4, 0), (6, 0, 1), (4, 2, 0), (3, 5, 0), (6, 1, 0),
    (4, 3, 0), (6, 1, 1), (4, 4, 0), (6, 2, 0), (6, 2, 1), (4, 5, 0), (6, 3, 0), (6, 3, 1),
    (6, 4, 0), (6, 4, 1), (6, 5, 0), (6, 5, 1),
)

def kernel(
    sizes,
    hidden_hbm,
    gain_hbm,
    weight_hbm,
    target_hbm,
    length_hbm,
    token_hbm,
    ensemble_hbm,
    centered_hbm,
    gathered,
    hidden_own,
    gain_own,
    weight_own,
    target_own,
    length_own,
    weight_turned,
    gain_wide,
    target_lanes,
    logits,
    normed,
    part,
    owned_y,
    owned_z,
    owned_score,
    stats_y,
    stats_z,
    scores,
    examples,
    token_out,
    ensemble_out,
    centered_out,
    load_sem,
    send_sem,
    recv_sem,
    stat_sem,
    end_sem,
    hello,
):
    ring, members, groups, batch, seq, width = sizes
    chunks = gathered.shape[0]
    units = chunks // 2
    depth = ring * ring * width
    vocab = weight_own.shape[1]
    s, d = lax.axis_index("seed"), lax.axis_index("dp")
    z, y = lax.axis_index("tensor_0"), lax.axis_index("tensor_1")

    def along_z(k):
        return lax.rem(z + (k + ring), ring)

    def along_y(k):
        return lax.rem(y + (k + ring), ring)

    loads = [
        pltpu.make_async_copy(hidden_hbm, hidden_own, load_sem.at[0]),
        pltpu.make_async_copy(target_hbm, target_own, load_sem.at[1]),
        pltpu.make_async_copy(gain_hbm, gain_own, load_sem.at[2]),
        pltpu.make_async_copy(length_hbm, length_own, load_sem.at[3]),
        pltpu.make_async_copy(weight_hbm, weight_own, load_sem.at[4]),
    ]
    loads[0].start()
    barrier = pltpu.get_barrier_semaphore()
    others = [(a, b) for a in range(members) for b in range(groups) if a or b]
    for k in (1, -1):
        pl.semaphore_signal(barrier, inc=1, device_id={"tensor_0": along_z(k)}, device_id_type=MESH)
        pl.semaphore_signal(barrier, inc=1, device_id={"tensor_1": along_y(k)}, device_id_type=MESH)


    def peer(a, b):
        return {"seed": lax.rem(s + a, members), "dp": lax.rem(d + b, groups)}

    beside = [(1, 0), (0, 1), (0, groups - 1)]
    for a, b in beside:
        pl.semaphore_signal(barrier, inc=1, device_id=peer(a, b), device_id_type=MESH)
    for load in loads[1:]:
        load.start()

    loads[0].wait()
    for q in range(batch // 4):
        joined = lanes_joined([hidden_own[4 * q + r].astype(jnp.float32) for r in range(4)])
        for r in range(3):
            gathered[3 * q + r, z, y] = joined[r].astype(jnp.bfloat16)
    pl.semaphore_wait(barrier, 4 + len(beside))

    sides = [(kind, sign) for kind in (0, 1) for sign in (1, -1)]

    arrival = {}

    def send(key, view, at, axis, sign):
        what, g, k = key
        if key not in arrival:
            arrival[key] = len(arrival)
        pltpu.make_async_remote_copy(
            src_ref=view(*at),
            dst_ref=view(*at),
            send_sem=send_sem.at[5 if (what, k) == (FIRST, 4) else what],
            recv_sem=recv_sem.at[arrival[key]],
            device_id={"tensor_0": along_z(sign)} if axis == 0 else {"tensor_1": along_y(sign)},
            device_id_type=MESH,
        ).start()

    def bulk(ref, which, number):
        return pltpu.make_async_remote_copy(
            src_ref=ref,
            dst_ref=ref,
            send_sem=send_sem.at[which],
            recv_sem=recv_sem.at[number],
            device_id={"tensor_0": along_z(1)},
            device_id_type=MESH,
        )

    waited = set()

    def need(what, g, k):
        if (what, g, k) in waited:
            return
        waited.add((what, g, k))
        if what in (FIRST, SECOND):
            ref = gathered.at[pl.ds(0, GROUPS[g][1]), 0, pl.ds(0, 2 if (what, k) == (FIRST, 4) else 4)]
        elif what == THIRD:
            ref = gathered.at[pl.ds(0, GROUPS[g][1]), pl.ds(0, 4)]
        else:
            ref = gathered.at[0, pl.ds(0, 4 if what == FOURTH else 2)]
        bulk(ref, what, arrival[what, g, k]).wait_recv()

    def wait_sends():
        refs = (
            gathered.at[:, 0, pl.ds(0, 6)],
            gathered.at[:, pl.ds(0, 2)],
            gathered.at[:, pl.ds(0, 2)],
            gathered.at[:, pl.ds(0, 2)],
            gathered.at[:, 0],
            gathered.at[:, 0, pl.ds(0, 1)],
        )
        for which, ref in enumerate(refs):
            bulk(ref, which, 0).wait_send()

    def place(kind, first, second):
        return (second, first) if kind == 0 else (first, second)

    def shards_at(kind, g, piece):
        begin, number = GROUPS[g]

        def view(dz, dy):
            return gathered.at[
                pl.ds(kind * units + begin, number), along_z(dz), along_y(dy), pl.ds(*piece)
            ]

        return view

    def block_at(kind, c, piece):
        def view(dz, dy):
            if kind == 0:
                return gathered.at[c, along_z(dz), pl.ds(*piece)]
            return gathered.at[units + c, pl.ds(*piece), along_y(dy)]

        return view

    group_of = {
        c: g for g, (begin, number) in enumerate(GROUPS) for c in range(begin, begin + number)
    }

    def transfer(what, g, k):
        if what == FIRST:
            if k > 1:
                need(FIRST, g, k - 1)
        elif what == SECOND:
            if k:
                need(FIRST, g, abs(k))
        elif what == THIRD:
            need(SECOND, g, k)
        elif what == FOURTH:
            need(THIRD, group_of[g], 0)
        else:
            need(FOURTH, g, 0)
        for kind, sign in sides:
            first_axis = 1 if kind == 0 else 0
            if what == FIRST:
                piece = (0, width) if k < 4 else ((0, width // 2), (width // 2, width // 2))[sign < 0]
                at, axis = place(kind, -(k - 1) * sign, 0), first_axis
                view = shards_at(kind, g, piece)
            elif what in (SECOND, THIRD):
                at, axis = place(kind, k, 0 if what == SECOND else -sign), 1 - first_axis
                view = shards_at(kind, g, (0, width))
            elif what == FOURTH:
                at, axis = place(kind, 0, -2 * sign), 1 - first_axis
                view = block_at(kind, g, (0, ring))
            else:
                at, axis = place(kind, 0, -3 * sign), 1 - first_axis
                view = block_at(kind, g, ((0, ring // 2), (ring // 2, ring // 2))[sign < 0])
            send((what, g, 0 if what == THIRD else k), view, at, axis, sign)

    steps = 4

    def prepare(k):
        if k == 0:
            for a, b in beside:
                pl.semaphore_signal(hello.at[0], inc=1, device_id=peer(a, b), device_id_type=MESH)
            for load in loads[1:]:
                load.wait()
            for q in range(batch // 4):
                joined = lanes_joined([target_own[pl.ds(4 * q + r, 1), :] for r in range(4)])
                for r in range(3):
                    target_lanes[pl.ds(3 * q + r, 1), :] = joined[r]
            for b in range(depth // LANES):
                row = gain_own[:, b * LANES : (b + 1) * LANES]
                gain_wide[b * LANES : (b + 1) * LANES, :] = jnp.broadcast_to(row, (LANES, LANES)).T
            for j in range(2 * OWNED, ring):
                part[j] = jnp.ones(part.shape[1:], jnp.float32)
        for b in range(k * depth // 256 // steps, (k + 1) * depth // 256 // steps):
            for v in range(vocab // 256):
                block = weight_own[b * 256 : (b + 1) * 256, v * 256 : (v + 1) * 256]
                weight_turned[v * 256 : (v + 1) * 256, b * 256 : (b + 1) * 256] = block.T

    def square_sum(u, side, ks):
        total = jnp.zeros((8, LANES), jnp.float32)
        for k in ks:
            x = gathered[u, along_z(k)] if side == 0 else gathered[units + u, :, along_y(k)]
            x = x.astype(jnp.float32).reshape(ring * width // 8, 8, LANES)
            total += jnp.sum(x * x, axis=0)
        return total

    def normalize(u):
        early = [square_sum(u, side, range(-3, 4)) for side in range(2)]
        need(FIFTH, u, 0)
        for side, c in enumerate((u, units + u)):
            total = jnp.sum(early[side] + square_sum(u, side, (4,)), axis=0, keepdims=True)
            scale = lax.rsqrt(total * (1.0 / depth) + RMS_EPSILON)
            for b in range(depth // 256):
                x = gathered[c, b].reshape(256, LANES).astype(jnp.float32)
                gain = gain_wide[b * 256 : (b + 1) * 256, :]
                normed[b * 256 : (b + 1) * 256, side * LANES : (side + 1) * LANES] = (
                    x * scale * gain
                ).astype(jnp.bfloat16)

    tiles = vocab // 256
    own_first = (z * ring + y) * vocab
    row = lax.broadcasted_iota(jnp.int32, (256, 2 * LANES), 0).reshape(32, 8, 2 * LANES)
    found = {}

    def dot(v):
        logits[v * 256 : (v + 1) * 256, :] = jnp.dot(
            weight_turned[v * 256 : (v + 1) * 256, :],
            normed[...],
            preferred_element_type=jnp.float32,
        )

    def stats(u, v):
        wanted = jnp.concatenate([target_lanes[pl.ds(c, 1), :] for c in (u, units + u)], axis=1)
        block = logits[v * 256 : (v + 1) * 256, :].reshape(32, 8, 2 * LANES)
        top = jnp.max(block, axis=0)
        scaled = jnp.exp(block - top[None])
        hit = row == (wanted - (own_first + v * 256))[None]
        other = jnp.where(hit, 0.0, scaled)
        found.setdefault(u, []).append(
            (
                top,
                jnp.sum(other, axis=0),
                jnp.sum(other * other, axis=0),
                jnp.sum(jnp.where(hit, scaled, 0.0), axis=0),
            )
        )

    def joined(u):
        top = functools.reduce(jnp.maximum, [f[0] for f in found[u]])
        top = jnp.max(top, axis=0, keepdims=True)
        scale = [jnp.exp(f[0] - top) for f in found[u]]
        value = [
            sum(f[1] * e for f, e in zip(found[u], scale)),
            sum(f[2] * (e * e) for f, e in zip(found[u], scale)),
            sum(f[3] * e for f, e in zip(found[u], scale)),
        ]
        value = [top] + [jnp.sum(x, axis=0, keepdims=True) for x in value]
        return [[x[:, side * LANES : (side + 1) * LANES] for x in value] for side in range(2)]

    def multiply(u):
        dot(0)
        late = 0 < u < units - 1
        if late:
            stats(u - 1, tiles - 1)
            before = joined(u - 1)
        for v in range(1, tiles):
            dot(v)
            stats(u, v - 1)
        if u >= units - 2:
            stats(u, tiles - 1)
            own = joined(u)
            after(u, own)
        if late:
            after(u - 1, before)

    def merged(parts, wide):
        tops = parts[:, :wide]
        top = jnp.max(tops, axis=0)
        scale = jnp.exp(tops - top[None])
        return (
            top,
            jnp.sum(parts[:, wide : 2 * wide] * scale, axis=0),
            jnp.sum(parts[:, 2 * wide : 3 * wide] * scale * scale, axis=0),
            jnp.sum(parts[:, 3 * wide : 4 * wide] * scale, axis=0),
        )

    def score_of(value):
        top, other, square, wanted = value
        return jnp.sqrt(other * other + square) / (other + wanted)

    near = sorted(range(1, ring), key=lambda k: -min(k, ring - k))

    def exchange(level, slot, source, target):
        mine = y if level == 0 else z

        def copy(src, dst, k):
            return pltpu.make_async_remote_copy(
                src_ref=src,
                dst_ref=dst,
                send_sem=stat_sem.at[0, slot],
                recv_sem=stat_sem.at[1, slot],
                device_id={"tensor_1": along_y(k)} if level == 0 else {"tensor_0": along_z(k)},
                device_id_type=MESH,
            )

        for k in near:
            copy(source(k), target(mine), k).start()
        seven = part.at[pl.ds(0, ring - 1)]
        return copy(seven, seven, 1)

    def share(u, level, value):
        buffer = stats_y if level == 0 else stats_z
        i = u - OWNED
        buffer[i, y if level == 0 else z] = jnp.concatenate(value, axis=0)
        mine = y if level == 0 else z
        return exchange(
            level, 2 * i + level, lambda k: buffer.at[i, mine], lambda p: buffer.at[i, p]
        )

    def tile(value):
        rows = jnp.concatenate(value, axis=0)
        return jnp.concatenate([rows, jnp.zeros((8 - rows.shape[0], LANES), jnp.float32)], axis=0)

    base = 2 * (units - OWNED)
    back = {}

    def after(u, rows):
        if u < OWNED:
            part[u] = tile(rows[0])
            part[OWNED + u] = tile(rows[1])
            if u == OWNED - 1:
                owned_y[y] = part[y]
                back["owned", 0] = exchange(
                    0, base, lambda k: part.at[along_y(k)], lambda p: owned_y.at[p]
                )
            return
        value = [jnp.concatenate([rows[0][k], rows[1][k]], axis=0) for k in range(4)]
        back[u, 0] = share(u, 0, value)

    def second_level(u):
        back[u, 0].wait_recv()
        back[u, 1] = share(u, 1, merged(stats_y[u - OWNED], 2))

    def finish(u):
        back[u, 1].wait_recv()
        score = score_of(merged(stats_z[u - OWNED], 2))
        scores[pl.ds(u, 1), :] = score[0:1]
        scores[pl.ds(units + u, 1), :] = score[1:2]

    for what, g, k in ORDER:
        if what == PREPARE:
            prepare(g)
        elif what == UNIT:
            if k == 0:
                if g == 0:
                    pl.semaphore_wait(hello.at[0], len(beside))
                    pl.semaphore_signal(hello.at[1], inc=1, device_id=peer(1, 0), device_id_type=MESH)
                normalize(g)
            elif k == 1:
                multiply(g)
        else:
            transfer(what, g, k)
    back["owned", 0].wait_recv()
    owned_z[z] = tile(merged(owned_y[...], 1))
    back["owned", 1] = exchange(1, base + 1, lambda k: owned_z.at[z], lambda p: owned_z.at[p])
    for u in range(OWNED, units):
        second_level(u)
    back["owned", 1].wait_recv()
    owned_score[y] = jnp.broadcast_to(score_of(merged(owned_z[...], 1)), (8, LANES))
    back["owned", 2] = exchange(
        0, base + 2, lambda k: owned_score.at[y], lambda p: owned_score.at[p]
    )
    example = lax.broadcasted_iota(jnp.int32, (batch, seq), 0)
    length = jnp.zeros((batch, seq), jnp.int32)
    for b in range(batch):
        length = jnp.where(example == b, length_own[b], length)
    valid = lax.broadcasted_iota(jnp.int32, (batch, seq), 1) < length
    wait_sends()
    for u in range(OWNED, units - 1):
        finish(u)
    back["owned", 2].wait_recv()
    for u in range(OWNED):
        scores[pl.ds(u, 1), :] = owned_score[u, 0:1, :]
        scores[pl.ds(units + u, 1), :] = owned_score[OWNED + u, 0:1, :]
    finish(units - 1)

    for q in range(batch // 4):
        row = [scores[pl.ds(3 * q + r, 1), :] for r in range(3)]
        split = [
            row[0][:, :seq],
            jnp.concatenate([row[0][:, 96:], row[1][:, :64]], axis=1),
            jnp.concatenate([row[1][:, 64:], row[2][:, :32]], axis=1),
            row[2][:, 32:],
        ]
        for r in range(4):
            token_out[pl.ds(4 * q + r, 1), :] = split[r]
    token = jnp.where(valid, token_out[...], 0.0)
    token_out[...] = token
    mean = jnp.sum(token, axis=1, keepdims=True) / length.astype(jnp.float32)[:, :1]
    examples[s * groups + d] = jnp.broadcast_to(mean, (batch, LANES))

    def end_copy(src, dst, a, b):
        return pltpu.make_async_remote_copy(
            src_ref=src,
            dst_ref=dst,
            send_sem=end_sem.at[0],
            recv_sem=end_sem.at[1],
            device_id=peer(a, b),
            device_id_type=MESH,
        )

    pl.semaphore_wait(hello.at[1], 1)
    own_place = s * groups + d
    for a, b in others:
        end_copy(examples.at[own_place], examples.at[own_place], a, b).start()
    rest = examples.at[pl.ds(0, len(others))]
    stores = [pltpu.make_async_copy(token_out, token_hbm, load_sem.at[5])]
    stores[0].start()
    end_copy(rest, rest, *others[0]).wait_recv()
    total = jnp.zeros((batch, LANES), jnp.float32)
    own = jnp.zeros((batch, LANES), jnp.float32)
    for b in range(groups):
        pair = examples[b]
        for a in range(1, members):
            pair += examples[a * groups + b]
        pair = pair * (1.0 / members)
        total += pair
        own = jnp.where(d == b, pair, own)
    average = jnp.sum(total, axis=0, keepdims=True) * (1.0 / (groups * batch))
    row = lax.broadcasted_iota(jnp.int32, (batch, LANES), 0)
    lane = lax.broadcasted_iota(jnp.int32, (batch, LANES), 1)
    ensemble = jnp.sum(jnp.where(row == lane, own, 0.0), axis=0, keepdims=True)
    ensemble_out[...] = ensemble[:, :batch]
    centered_out[...] = (ensemble - average)[:, :batch]
    stores.append(pltpu.make_async_copy(ensemble_out, ensemble_hbm, load_sem.at[6]))
    stores.append(pltpu.make_async_copy(centered_out, centered_hbm, load_sem.at[7]))
    for store in stores[1:]:
        store.start()
    end_copy(rest, rest, *others[0]).wait_send()
    for copy in back.values():
        copy.wait_send()
    for store in stores:
        store.wait()


def lanes_joined(part):
    return (
        jnp.concatenate([part[0], part[1][:, :32]], axis=1),
        jnp.concatenate([part[1][:, 32:], part[2][:, :64]], axis=1),
        jnp.concatenate([part[2][:, 64:], part[3]], axis=1),
    )


def hand_over(*refs):
    count = len(refs) // 2
    copies = [
        pltpu.make_async_copy(refs[k], refs[count + k], refs[-1].at[k]) for k in range(count)
    ]
    for copy in copies:
        copy.start()
    for copy in copies:
        copy.wait()


def shards(members, groups, hidden, norm_gain, lm_head, targets, lengths):
    batch, seq, width = hidden.shape[1:]
    depth, vocab = lm_head.shape[1:]
    chunks = batch * seq // LANES
    units = chunks // 2
    direct = units - OWNED
    far = pl.BlockSpec(memory_space=pl.ANY)
    f32 = jnp.float32
    outs = (
        jax.ShapeDtypeStruct((batch, seq), f32),
        jax.ShapeDtypeStruct((1, batch), f32),
        jax.ShapeDtypeStruct((1, batch), f32),
    )
    result = pl.pallas_call(
        functools.partial(kernel, (RING, members, groups, batch, seq, width)),
        out_shape=outs,
        in_specs=[far] * 5,
        out_specs=(far, far, far),
        scratch_shapes=[
            pltpu.VMEM((chunks, RING, RING, width, LANES), jnp.bfloat16),
            pltpu.VMEM((batch, width, seq), jnp.bfloat16),
            pltpu.VMEM((1, depth), f32),
            pltpu.VMEM((depth, vocab), jnp.bfloat16),
            pltpu.VMEM((batch, seq), jnp.int32),
            pltpu.SMEM((batch,), jnp.int32),
            pltpu.VMEM((vocab, depth), jnp.bfloat16),
            pltpu.VMEM((depth, LANES), f32),
            pltpu.VMEM((chunks, LANES), jnp.int32),
            pltpu.VMEM((vocab, 2 * LANES), f32),
            pltpu.VMEM((depth, 2 * LANES), jnp.bfloat16),
            pltpu.VMEM((RING, 8, LANES), f32),
            pltpu.VMEM((RING, 8, LANES), f32),
            pltpu.VMEM((RING, 8, LANES), f32),
            pltpu.VMEM((RING, 8, LANES), f32),
            pltpu.VMEM((direct, RING, 8, LANES), f32),
            pltpu.VMEM((direct, RING, 8, LANES), f32),
            pltpu.VMEM((chunks, LANES), f32),
            pltpu.VMEM((members * groups, batch, LANES), f32),
            pltpu.VMEM((batch, seq), f32),
            pltpu.VMEM((1, batch), f32),
            pltpu.VMEM((1, batch), f32),
            pltpu.SemaphoreType.DMA((8,)),
            pltpu.SemaphoreType.DMA((6,)),
            pltpu.SemaphoreType.DMA((13 * len(GROUPS) + 2 * units,)),
            pltpu.SemaphoreType.DMA((2, 2 * direct + 3)),
            pltpu.SemaphoreType.DMA((2,)),
            pltpu.SemaphoreType.REGULAR((2,)),
        ],
        compiler_params=pltpu.CompilerParams(
            collective_id=0, has_side_effects=True, vmem_limit_bytes=67043328
        ),
    )(
        hidden[0].transpose(0, 2, 1),
        norm_gain,
        lm_head[0],
        targets,
        lengths,
    )
    token, ensemble, centered = pl.pallas_call(
        hand_over,
        out_shape=outs,
        in_specs=[far] * 3,
        out_specs=(far, far, far),
        scratch_shapes=[pltpu.SemaphoreType.DMA((3,))],
    )(*result)
    return token[None], ensemble[0], centered[0]


def solution(mesh):
    finer = Mesh(
        mesh.devices.reshape(mesh.shape["seed"], mesh.shape["dp"], RING, RING),
        ("seed", "dp", "tensor_0", "tensor_1"),
    )
    in_specs = (
        P("seed", "dp", None, TENSOR),
        P("seed", None),
        P("seed", None, TENSOR),
        P("dp", None),
        P("dp"),
    )
    out_specs = (P("seed", "dp", None), P("dp"), P("dp"))
    return jax.shard_map(
        functools.partial(shards, mesh.shape["seed"], mesh.shape["dp"]),
        mesh=finer,
        in_specs=in_specs,
        out_specs=out_specs,
        check_vma=False,
    )
```

```python
import functools

import jax
import jax.numpy as jnp
from jax import lax
from jax.experimental import pallas as pl
from jax.experimental.pallas import tpu as pltpu
from jax.sharding import Mesh
from jax.sharding import PartitionSpec as P

MESH = pl.DeviceIdType.MESH
TENSOR = ("tensor_0", "tensor_1")
LANES = 128
RMS_EPSILON = 1e-05
RING = 8
FIRST, SECOND, THIRD, FOURTH, FIFTH, PREPARE, UNIT = range(7)
OWNED = 2

GROUPS = ((0, 2), (2, 4))
ORDER = (
    (0, 0, 1), (0, 1, 1), (5, 0, 0), (1, 1, 0), (5, 1, 0), (5, 2, 0), (1, 0, 0), (5, 3, 0),
    (0, 0, 2), (1, 0, -1), (1, 0, 1), (0, 1, 2), (1, 1, -1), (2, 0, 0), (2, 1, 0), (0, 0, 3),
    (2, 0, -1), (2, 0, 1), (1, 0, -2), (0, 1, 3), (1, 1, 2), (1, 1, -2), (0, 0, 4), (1, 0, 3),
    (1, 0, -3), (1, 0, 2), (2, 0, -2), (2, 1, -1), (0, 1, 4), (1, 1, 3), (1, 0, 4), (2, 0, 3),
    (2, 0, -3), (2, 0, 2), (1, 1, -3), (2, 1, 2), (1, 1, 4), (2, 0, 4), (2, 1, 3), (1, 1, 1),
    (2, 1, -3), (2, 1, -2), (2, 1, 4), (3, 0, 0), (2, 1, 1), (3, 1, 0), (4, 0, 0), (3, 2, 0),
    (3, 3, 0), (4, 1, 0), (6, 0, 0), (3, 4, 0), (6, 0, 1), (4, 2, 0), (3, 5, 0), (6, 1, 0),
    (4, 3, 0), (6, 1, 1), (4, 4, 0), (6, 2, 0), (6, 2, 1), (4, 5, 0), (6, 3, 0), (6, 3, 1),
    (6, 4, 0), (6, 4, 1), (6, 5, 0), (6, 5, 1),
)

def kernel(
    sizes,
    hidden_hbm,
    gain_hbm,
    weight_hbm,
    target_hbm,
    length_hbm,
    token_hbm,
    ensemble_hbm,
    centered_hbm,
    gathered,
    hidden_own,
    gain_own,
    weight_own,
    target_own,
    length_own,
    weight_turned,
    gain_wide,
    target_lanes,
    logits,
    normed,
    part,
    owned_y,
    owned_z,
    owned_score,
    stats_y,
    stats_z,
    scores,
    examples,
    token_out,
    ensemble_out,
    centered_out,
    load_sem,
    send_sem,
    recv_sem,
    stat_sem,
    end_sem,
    hello,
):
    ring, members, groups, batch, seq, width = sizes
    chunks = gathered.shape[0]
    units = chunks // 2
    depth = ring * ring * width
    vocab = weight_own.shape[1]
    s, d = lax.axis_index("seed"), lax.axis_index("dp")
    z, y = lax.axis_index("tensor_0"), lax.axis_index("tensor_1")

    def along_z(k):
        return lax.rem(z + (k + ring), ring)

    def along_y(k):
        return lax.rem(y + (k + ring), ring)

    loads = [
        pltpu.make_async_copy(hidden_hbm, hidden_own, load_sem.at[0]),
        pltpu.make_async_copy(target_hbm, target_own, load_sem.at[1]),
        pltpu.make_async_copy(gain_hbm, gain_own, load_sem.at[2]),
        pltpu.make_async_copy(length_hbm, length_own, load_sem.at[3]),
        pltpu.make_async_copy(weight_hbm, weight_own, load_sem.at[4]),
    ]
    loads[0].start()
    barrier = pltpu.get_barrier_semaphore()
    others = [(a, b) for a in range(members) for b in range(groups) if a or b]
    for k in (1, -1):
        pl.semaphore_signal(barrier, inc=1, device_id={"tensor_0": along_z(k)}, device_id_type=MESH)
        pl.semaphore_signal(barrier, inc=1, device_id={"tensor_1": along_y(k)}, device_id_type=MESH)


    def peer(a, b):
        return {"seed": lax.rem(s + a, members), "dp": lax.rem(d + b, groups)}

    beside = [(1, 0), (0, 1), (0, groups - 1)]
    for a, b in beside:
        pl.semaphore_signal(barrier, inc=1, device_id=peer(a, b), device_id_type=MESH)
    for load in loads[1:]:
        load.start()

    loads[0].wait()
    for q in range(batch // 4):
        joined = lanes_joined([hidden_own[4 * q + r].astype(jnp.float32) for r in range(4)])
        for r in range(3):
            gathered[3 * q + r, z, y] = joined[r].astype(jnp.bfloat16)
    pl.semaphore_wait(barrier, 4 + len(beside))

    sides = [(kind, sign) for kind in (0, 1) for sign in (1, -1)]

    arrival = {}

    def send(key, view, at, axis, sign):
        what, g, k = key
        if key not in arrival:
            arrival[key] = len(arrival)
        pltpu.make_async_remote_copy(
            src_ref=view(*at),
            dst_ref=view(*at),
            send_sem=send_sem.at[5 if (what, k) == (FIRST, 4) else what],
            recv_sem=recv_sem.at[arrival[key]],
            device_id={"tensor_0": along_z(sign)} if axis == 0 else {"tensor_1": along_y(sign)},
            device_id_type=MESH,
        ).start()

    def bulk(ref, which, number):
        return pltpu.make_async_remote_copy(
            src_ref=ref,
            dst_ref=ref,
            send_sem=send_sem.at[which],
            recv_sem=recv_sem.at[number],
            device_id={"tensor_0": along_z(1)},
            device_id_type=MESH,
        )

    waited = set()

    def need(what, g, k):
        if (what, g, k) in waited:
            return
        waited.add((what, g, k))
        if what in (FIRST, SECOND):
            ref = gathered.at[pl.ds(0, GROUPS[g][1]), 0, pl.ds(0, 2 if (what, k) == (FIRST, 4) else 4)]
        elif what == THIRD:
            ref = gathered.at[pl.ds(0, GROUPS[g][1]), pl.ds(0, 4)]
        else:
            ref = gathered.at[0, pl.ds(0, 4 if what == FOURTH else 2)]
        bulk(ref, what, arrival[what, g, k]).wait_recv()

    def wait_sends():
        refs = (
            gathered.at[:, 0, pl.ds(0, 6)],
            gathered.at[:, pl.ds(0, 2)],
            gathered.at[:, pl.ds(0, 2)],
            gathered.at[:, pl.ds(0, 2)],
            gathered.at[:, 0],
            gathered.at[:, 0, pl.ds(0, 1)],
        )
        for which, ref in enumerate(refs):
            bulk(ref, which, 0).wait_send()

    def place(kind, first, second):
        return (second, first) if kind == 0 else (first, second)

    def shards_at(kind, g, piece):
        begin, number = GROUPS[g]

        def view(dz, dy):
            return gathered.at[
                pl.ds(kind * units + begin, number), along_z(dz), along_y(dy), pl.ds(*piece)
            ]

        return view

    def block_at(kind, c, piece):
        def view(dz, dy):
            if kind == 0:
                return gathered.at[c, along_z(dz), pl.ds(*piece)]
            return gathered.at[units + c, pl.ds(*piece), along_y(dy)]

        return view

    group_of = {
        c: g for g, (begin, number) in enumerate(GROUPS) for c in range(begin, begin + number)
    }

    def transfer(what, g, k):
        if what == FIRST:
            if k > 1:
                need(FIRST, g, k - 1)
        elif what == SECOND:
            if k:
                need(FIRST, g, abs(k))
        elif what == THIRD:
            need(SECOND, g, k)
        elif what == FOURTH:
            need(THIRD, group_of[g], 0)
        else:
            need(FOURTH, g, 0)
        for kind, sign in sides:
            first_axis = 1 if kind == 0 else 0
            if what == FIRST:
                piece = (0, width) if k < 4 else ((0, width // 2), (width // 2, width // 2))[sign < 0]
                at, axis = place(kind, -(k - 1) * sign, 0), first_axis
                view = shards_at(kind, g, piece)
            elif what in (SECOND, THIRD):
                at, axis = place(kind, k, 0 if what == SECOND else -sign), 1 - first_axis
                view = shards_at(kind, g, (0, width))
            elif what == FOURTH:
                at, axis = place(kind, 0, -2 * sign), 1 - first_axis
                view = block_at(kind, g, (0, ring))
            else:
                at, axis = place(kind, 0, -3 * sign), 1 - first_axis
                view = block_at(kind, g, ((0, ring // 2), (ring // 2, ring // 2))[sign < 0])
            send((what, g, 0 if what == THIRD else k), view, at, axis, sign)

    steps = 4

    def prepare(k):
        if k == 0:
            for a, b in beside:
                pl.semaphore_signal(hello.at[0], inc=1, device_id=peer(a, b), device_id_type=MESH)
            for load in loads[1:]:
                load.wait()
            for q in range(batch // 4):
                joined = lanes_joined([target_own[pl.ds(4 * q + r, 1), :] for r in range(4)])
                for r in range(3):
                    target_lanes[pl.ds(3 * q + r, 1), :] = joined[r]
            for b in range(depth // LANES):
                row = gain_own[:, b * LANES : (b + 1) * LANES]
                gain_wide[b * LANES : (b + 1) * LANES, :] = jnp.broadcast_to(row, (LANES, LANES)).T
            for j in range(2 * OWNED, ring):
                part[j] = jnp.ones(part.shape[1:], jnp.float32)
        for b in range(k * depth // 256 // steps, (k + 1) * depth // 256 // steps):
            for v in range(vocab // 256):
                block = weight_own[b * 256 : (b + 1) * 256, v * 256 : (v + 1) * 256]
                weight_turned[v * 256 : (v + 1) * 256, b * 256 : (b + 1) * 256] = block.T

    def square_sum(u, side, ks):
        total = jnp.zeros((8, LANES), jnp.float32)
        for k in ks:
            x = gathered[u, along_z(k)] if side == 0 else gathered[units + u, :, along_y(k)]
            x = x.astype(jnp.float32).reshape(ring * width // 8, 8, LANES)
            total += jnp.sum(x * x, axis=0)
        return total

    def normalize(u):
        early = [square_sum(u, side, range(-3, 4)) for side in range(2)]
        need(FIFTH, u, 0)
        for side, c in enumerate((u, units + u)):
            total = jnp.sum(early[side] + square_sum(u, side, (4,)), axis=0, keepdims=True)
            scale = lax.rsqrt(total * (1.0 / depth) + RMS_EPSILON)
            for b in range(depth // 256):
                x = gathered[c, b].reshape(256, LANES).astype(jnp.float32)
                gain = gain_wide[b * 256 : (b + 1) * 256, :]
                normed[b * 256 : (b + 1) * 256, side * LANES : (side + 1) * LANES] = (
                    x * scale * gain
                ).astype(jnp.bfloat16)

    tiles = vocab // 256
    own_first = (z * ring + y) * vocab
    row = lax.broadcasted_iota(jnp.int32, (256, 2 * LANES), 0).reshape(32, 8, 2 * LANES)
    found = {}

    def dot(v):
        logits[v * 256 : (v + 1) * 256, :] = jnp.dot(
            weight_turned[v * 256 : (v + 1) * 256, :],
            normed[...],
            preferred_element_type=jnp.float32,
        )

    def stats(u, v):
        wanted = jnp.concatenate([target_lanes[pl.ds(c, 1), :] for c in (u, units + u)], axis=1)
        block = logits[v * 256 : (v + 1) * 256, :].reshape(32, 8, 2 * LANES)
        top = jnp.max(block, axis=0)
        scaled = jnp.exp(block - top[None])
        hit = row == (wanted - (own_first + v * 256))[None]
        other = jnp.where(hit, 0.0, scaled)
        found.setdefault(u, []).append(
            (
                top,
                jnp.sum(other, axis=0),
                jnp.sum(other * other, axis=0),
                jnp.sum(jnp.where(hit, scaled, 0.0), axis=0),
            )
        )

    def joined(u):
        top = functools.reduce(jnp.maximum, [f[0] for f in found[u]])
        top = jnp.max(top, axis=0, keepdims=True)
        scale = [jnp.exp(f[0] - top) for f in found[u]]
        value = [
            sum(f[1] * e for f, e in zip(found[u], scale)),
            sum(f[2] * (e * e) for f, e in zip(found[u], scale)),
            sum(f[3] * e for f, e in zip(found[u], scale)),
        ]
        value = [top] + [jnp.sum(x, axis=0, keepdims=True) for x in value]
        return [[x[:, side * LANES : (side + 1) * LANES] for x in value] for side in range(2)]

    def multiply(u):
        dot(0)
        late = 0 < u < units - 1
        if late:
            stats(u - 1, tiles - 1)
            before = joined(u - 1)
        for v in range(1, tiles):
            dot(v)
            stats(u, v - 1)
        if u >= units - 2:
            stats(u, tiles - 1)
            own = joined(u)
            after(u, own)
        if late:
            after(u - 1, before)

    def merged(parts, wide):
        tops = parts[:, :wide]
        top = jnp.max(tops, axis=0)
        scale = jnp.exp(tops - top[None])
        return (
            top,
            jnp.sum(parts[:, wide : 2 * wide] * scale, axis=0),
            jnp.sum(parts[:, 2 * wide : 3 * wide] * scale * scale, axis=0),
            jnp.sum(parts[:, 3 * wide : 4 * wide] * scale, axis=0),
        )

    def score_of(value):
        top, other, square, wanted = value
        return jnp.sqrt(other * other + square) / (other + wanted)

    near = sorted(range(1, ring), key=lambda k: -min(k, ring - k))

    def exchange(level, slot, source, target):
        mine = y if level == 0 else z

        def copy(src, dst, k):
            return pltpu.make_async_remote_copy(
                src_ref=src,
                dst_ref=dst,
                send_sem=stat_sem.at[0, slot],
                recv_sem=stat_sem.at[1, slot],
                device_id={"tensor_1": along_y(k)} if level == 0 else {"tensor_0": along_z(k)},
                device_id_type=MESH,
            )

        for k in near:
            copy(source(k), target(mine), k).start()
        seven = part.at[pl.ds(0, ring - 1)]
        return copy(seven, seven, 1)

    def share(u, level, value):
        buffer = stats_y if level == 0 else stats_z
        i = u - OWNED
        buffer[i, y if level == 0 else z] = jnp.concatenate(value, axis=0)
        mine = y if level == 0 else z
        return exchange(
            level, 2 * i + level, lambda k: buffer.at[i, mine], lambda p: buffer.at[i, p]
        )

    def tile(value):
        rows = jnp.concatenate(value, axis=0)
        return jnp.concatenate([rows, jnp.zeros((8 - rows.shape[0], LANES), jnp.float32)], axis=0)

    base = 2 * (units - OWNED)
    back = {}

    def after(u, rows):
        if u < OWNED:
            part[u] = tile(rows[0])
            part[OWNED + u] = tile(rows[1])
            if u == OWNED - 1:
                owned_y[y] = part[y]
                back["owned", 0] = exchange(
                    0, base, lambda k: part.at[along_y(k)], lambda p: owned_y.at[p]
                )
            return
        value = [jnp.concatenate([rows[0][k], rows[1][k]], axis=0) for k in range(4)]
        back[u, 0] = share(u, 0, value)

    def second_level(u):
        back[u, 0].wait_recv()
        back[u, 1] = share(u, 1, merged(stats_y[u - OWNED], 2))

    def finish(u):
        back[u, 1].wait_recv()
        score = score_of(merged(stats_z[u - OWNED], 2))
        scores[pl.ds(u, 1), :] = score[0:1]
        scores[pl.ds(units + u, 1), :] = score[1:2]

    for what, g, k in ORDER:
        if what == PREPARE:
            prepare(g)
        elif what == UNIT:
            if k == 0:
                if g == 0:
                    pl.semaphore_wait(hello.at[0], len(beside))
                    pl.semaphore_signal(hello.at[1], inc=1, device_id=peer(1, 0), device_id_type=MESH)
                normalize(g)
            elif k == 1:
                multiply(g)
        else:
            transfer(what, g, k)
    back["owned", 0].wait_recv()
    owned_z[z] = tile(merged(owned_y[...], 1))
    back["owned", 1] = exchange(1, base + 1, lambda k: owned_z.at[z], lambda p: owned_z.at[p])
    for u in range(OWNED, units):
        second_level(u)
    back["owned", 1].wait_recv()
    owned_score[y] = jnp.broadcast_to(score_of(merged(owned_z[...], 1)), (8, LANES))
    back["owned", 2] = exchange(
        0, base + 2, lambda k: owned_score.at[y], lambda p: owned_score.at[p]
    )
    example = lax.broadcasted_iota(jnp.int32, (batch, seq), 0)
    length = jnp.zeros((batch, seq), jnp.int32)
    for b in range(batch):
        length = jnp.where(example == b, length_own[b], length)
    valid = lax.broadcasted_iota(jnp.int32, (batch, seq), 1) < length
    wait_sends()
    for u in range(OWNED, units - 1):
        finish(u)
    back["owned", 2].wait_recv()
    for u in range(OWNED):
        scores[pl.ds(u, 1), :] = owned_score[u, 0:1, :]
        scores[pl.ds(units + u, 1), :] = owned_score[OWNED + u, 0:1, :]
    finish(units - 1)

    for q in range(batch // 4):
        row = [scores[pl.ds(3 * q + r, 1), :] for r in range(3)]
        split = [
            row[0][:, :seq],
            jnp.concatenate([row[0][:, 96:], row[1][:, :64]], axis=1),
            jnp.concatenate([row[1][:, 64:], row[2][:, :32]], axis=1),
            row[2][:, 32:],
        ]
        for r in range(4):
            token_out[pl.ds(4 * q + r, 1), :] = split[r]
    token = jnp.where(valid, token_out[...], 0.0)
    token_out[...] = token
    mean = jnp.sum(token, axis=1, keepdims=True) / length.astype(jnp.float32)[:, :1]
    diagonal = lax.broadcasted_iota(jnp.int32, (batch, LANES), 0) == lax.broadcasted_iota(
        jnp.int32, (batch, LANES), 1
    )
    examples[s * groups + d] = jnp.sum(
        jnp.where(diagonal, jnp.broadcast_to(mean, (batch, LANES)), 0.0), axis=0, keepdims=True
    )

    def end_copy(src, dst, a, b):
        return pltpu.make_async_remote_copy(
            src_ref=src,
            dst_ref=dst,
            send_sem=end_sem.at[0],
            recv_sem=end_sem.at[1],
            device_id=peer(a, b),
            device_id_type=MESH,
        )

    pl.semaphore_wait(hello.at[1], 1)
    own_place = s * groups + d
    for a, b in others:
        end_copy(examples.at[own_place], examples.at[own_place], a, b).start()
    rest = examples.at[pl.ds(0, len(others))]
    stores = [pltpu.make_async_copy(token_out, token_hbm, load_sem.at[5])]
    stores[0].start()
    end_copy(rest, rest, *others[0]).wait_recv()
    total = jnp.zeros((1, LANES), jnp.float32)
    ensemble = jnp.zeros((1, LANES), jnp.float32)
    for b in range(groups):
        pair = examples[b]
        for a in range(1, members):
            pair += examples[a * groups + b]
        pair = pair * (1.0 / members)
        total += pair
        ensemble = jnp.where(d == b, pair, ensemble)
    average = jnp.sum(total, axis=1, keepdims=True) * (1.0 / (groups * batch))
    ensemble_out[...] = ensemble[:, :batch]
    centered_out[...] = (ensemble - average)[:, :batch]
    stores.append(pltpu.make_async_copy(ensemble_out, ensemble_hbm, load_sem.at[6]))
    stores.append(pltpu.make_async_copy(centered_out, centered_hbm, load_sem.at[7]))
    for store in stores[1:]:
        store.start()
    end_copy(rest, rest, *others[0]).wait_send()
    for copy in back.values():
        copy.wait_send()
    for store in stores:
        store.wait()


def lanes_joined(part):
    return (
        jnp.concatenate([part[0], part[1][:, :32]], axis=1),
        jnp.concatenate([part[1][:, 32:], part[2][:, :64]], axis=1),
        jnp.concatenate([part[2][:, 64:], part[3]], axis=1),
    )


def hand_over(*refs):
    count = len(refs) // 2
    copies = [
        pltpu.make_async_copy(refs[k], refs[count + k], refs[-1].at[k]) for k in range(count)
    ]
    for copy in copies:
        copy.start()
    for copy in copies:
        copy.wait()


def shards(members, groups, hidden, norm_gain, lm_head, targets, lengths):
    batch, seq, width = hidden.shape[1:]
    depth, vocab = lm_head.shape[1:]
    chunks = batch * seq // LANES
    units = chunks // 2
    direct = units - OWNED
    far = pl.BlockSpec(memory_space=pl.ANY)
    f32 = jnp.float32
    outs = (
        jax.ShapeDtypeStruct((batch, seq), f32),
        jax.ShapeDtypeStruct((1, batch), f32),
        jax.ShapeDtypeStruct((1, batch), f32),
    )
    result = pl.pallas_call(
        functools.partial(kernel, (RING, members, groups, batch, seq, width)),
        out_shape=outs,
        in_specs=[far] * 5,
        out_specs=(far, far, far),
        scratch_shapes=[
            pltpu.VMEM((chunks, RING, RING, width, LANES), jnp.bfloat16),
            pltpu.VMEM((batch, width, seq), jnp.bfloat16),
            pltpu.VMEM((1, depth), f32),
            pltpu.VMEM((depth, vocab), jnp.bfloat16),
            pltpu.VMEM((batch, seq), jnp.int32),
            pltpu.SMEM((batch,), jnp.int32),
            pltpu.VMEM((vocab, depth), jnp.bfloat16),
            pltpu.VMEM((depth, LANES), f32),
            pltpu.VMEM((chunks, LANES), jnp.int32),
            pltpu.VMEM((vocab, 2 * LANES), f32),
            pltpu.VMEM((depth, 2 * LANES), jnp.bfloat16),
            pltpu.VMEM((RING, 8, LANES), f32),
            pltpu.VMEM((RING, 8, LANES), f32),
            pltpu.VMEM((RING, 8, LANES), f32),
            pltpu.VMEM((RING, 8, LANES), f32),
            pltpu.VMEM((direct, RING, 8, LANES), f32),
            pltpu.VMEM((direct, RING, 8, LANES), f32),
            pltpu.VMEM((chunks, LANES), f32),
            pltpu.VMEM((members * groups, 1, LANES), f32),
            pltpu.VMEM((batch, seq), f32),
            pltpu.VMEM((1, batch), f32),
            pltpu.VMEM((1, batch), f32),
            pltpu.SemaphoreType.DMA((8,)),
            pltpu.SemaphoreType.DMA((6,)),
            pltpu.SemaphoreType.DMA((13 * len(GROUPS) + 2 * units,)),
            pltpu.SemaphoreType.DMA((2, 2 * direct + 3)),
            pltpu.SemaphoreType.DMA((2,)),
            pltpu.SemaphoreType.REGULAR((2,)),
        ],
        compiler_params=pltpu.CompilerParams(
            collective_id=0, has_side_effects=True, vmem_limit_bytes=67043328
        ),
    )(
        hidden[0].transpose(0, 2, 1),
        norm_gain,
        lm_head[0],
        targets,
        lengths,
    )
    token, ensemble, centered = pl.pallas_call(
        hand_over,
        out_shape=outs,
        in_specs=[far] * 3,
        out_specs=(far, far, far),
        scratch_shapes=[pltpu.SemaphoreType.DMA((3,))],
    )(*result)
    return token[None], ensemble[0], centered[0]


def solution(mesh):
    finer = Mesh(
        mesh.devices.reshape(mesh.shape["seed"], mesh.shape["dp"], RING, RING),
        ("seed", "dp", "tensor_0", "tensor_1"),
    )
    in_specs = (
        P("seed", "dp", None, TENSOR),
        P("seed", None),
        P("seed", None, TENSOR),
        P("dp", None),
        P("dp"),
    )
    out_specs = (P("seed", "dp", None), P("dp"), P("dp"))
    return jax.shard_map(
        functools.partial(shards, mesh.shape["seed"], mesh.shape["dp"]),
        mesh=finer,
        in_specs=in_specs,
        out_specs=out_specs,
        check_vma=False,
    )
```
